32 devices in a mesh: dp: 4 (over x, core), mp: 8 (over z, y).
Axes of the slice: x: 2, y: 2, z: 4, core: 2. Of those that a mesh axis runs over, the one named last changes fastest.
Arguments:
- tokens: bfloat16 [128, 8192], P('dp', 'mp'), may hold values from -6 to 6
- gate_up_weight: bfloat16 [2, 8192, 15360], P(None, 'mp', 'dp'), may hold values from -0.0625 to 0.0625
- down_weight: bfloat16 [15360, 8192], P('dp', 'mp'), may hold values from -0.046875 to 0.046875
- gate_up_input_factor: bfloat16 [2, 8192, 64], P(None, 'mp'), may hold values from -0.0625 to 0.0625
- gate_up_output_factor: bfloat16 [2, 64, 15360], P(None, None, 'dp'), may hold values from -0.046875 to 0.046875
- down_input_factor: bfloat16 [15360, 64], P('dp'), may hold values from -0.046875 to 0.046875
- down_output_factor: bfloat16 [64, 8192], P(None, 'mp'), may hold values from -0.0625 to 0.0625
- cotangent: bfloat16 [128, 8192], P('dp', 'mp'), may hold values from -6 to 6
Outputs:
- output: bfloat16 [128, 8192], P('dp', 'mp')
- input_grad: bfloat16 [128, 8192], P('dp', 'mp')
- grad_gate_up_lower: float32 [2, 8192, 64], P(None, 'mp')
- gate_up_output_factor_gradient: float32 [2, 64, 15360], P(None, None, 'dp')
- down_input_factor_gradient: float32 [15360, 64], P('dp')
- down_output_factor_gradient: float32 [64, 8192], P(None, 'mp')
The draws below stay inside these ranges and needn't reach their ends.
All inputs are finite; a program needn't handle non-finite values.
Results may differ from the reference program's by a relative error of at most 0.0065.
Values may be sent and summed in bfloat16 or wider, within the bound.
No kernel may reach another device: no remote copies, remote signals or barrier semaphores. Data moves between devices by JAX's collectives and lax.ppermute only.
A program may use at most 64 MiB of HBM per device.

```python
import jax
import jax.numpy as jnp
from jax import lax

D = 8192
FF = 15360
R = 64
TOKENS = 128


def steps_of(key, dims, cuts, low, high):
    loudness = 1.0
    for dim, parts in cuts:
        draws = jax.random.uniform(jax.random.fold_in(jax.random.fold_in(key, 6), dim), (parts,), jnp.float32, low / len(cuts), high / len(cuts))
        loudness = loudness * jnp.repeat(jnp.exp(draws), dims[dim] // parts).reshape((-1,) + (1,) * (len(dims) - 1 - dim))
    return loudness


def normal_values(stream_key, shape, width, bound, split=(), dtype=jnp.bfloat16):
    gain = steps_of(stream_key, shape, split, -0.22, 0.18) if split else 1.0
    values = jax.random.normal(stream_key, shape, jnp.float32) * width * gain
    return jnp.minimum(jnp.maximum(values, -bound), bound).astype(dtype)


def setup_inputs(seed: int = 0) -> dict:
    key_of = jax.random.split(jax.random.key(seed), 9)
    tokens = normal_values(key_of[0], (TOKENS, D), 1.0, 6.0, ((0, 4), (1, 8)))
    gate_up_weight = normal_values(key_of[1], (2, D, FF), D ** -0.5, 0.0625, ((1, 8), (2, 4)))
    down_weight = normal_values(key_of[2], (FF, D), FF ** -0.5, 0.046875, ((0, 4), (1, 8)))
    gate_up_input_factor = normal_values(key_of[3], (2, D, R), D ** -0.5, 0.0625, ((1, 8),))
    gate_up_output_factor = normal_values(key_of[4], (2, R, FF), FF ** -0.5, 0.046875, ((2, 4),))
    down_input_factor = normal_values(key_of[5], (FF, R), FF ** -0.5, 0.046875, ((0, 4),))
    down_output_factor = normal_values(key_of[6], (R, D), D ** -0.5, 0.0625, ((1, 8),))
    cotangent = normal_values(key_of[7], (TOKENS, D), 1.0, 6.0, ((0, 4), (1, 8)))
    return {"tokens": tokens, "gate_up_weight": gate_up_weight, "down_weight": down_weight, "gate_up_input_factor": gate_up_input_factor, "gate_up_output_factor": gate_up_output_factor, "down_input_factor": down_input_factor, "down_output_factor": down_output_factor, "cotangent": cotangent}


adapter_scale = 2.0


def reference(tokens, gate_up_weight, down_weight, gate_up_input_factor, gate_up_output_factor, down_input_factor, down_output_factor, cotangent):
    single_float = jnp.float32
    upper_projection = lax.Precision.HIGHEST
    scale_factor = TOKENS ** -0.5
    lower_results = []
    pres = []
    for rank_dimension in range(2):
        lower_projection = jnp.dot(tokens, gate_up_input_factor[rank_dimension], preferred_element_type=single_float)
        lower_results.append(lower_projection)
        preactivation = jnp.dot(tokens, gate_up_weight[rank_dimension], preferred_element_type=single_float)
        preactivation = preactivation + adapter_scale * jnp.dot(lower_projection, gate_up_output_factor[rank_dimension].astype(single_float), precision=upper_projection)
        pres.append(preactivation)
    gate, upper = pres[0], pres[1]
    hidden_state = (jax.nn.silu(gate) * upper).astype(jnp.bfloat16)
    lower_down_projection = jnp.dot(hidden_state, down_input_factor, preferred_element_type=single_float)
    output = jnp.dot(hidden_state, down_weight, preferred_element_type=single_float)
    output = output + adapter_scale * jnp.dot(lower_down_projection, down_output_factor.astype(single_float), precision=upper_projection)
    output = output.astype(jnp.bfloat16)
    backward_down_rows = jnp.dot(cotangent, down_output_factor.T, preferred_element_type=single_float).astype(jnp.bfloat16)
    hidden_state_gradient = jnp.dot(cotangent, down_weight.T, preferred_element_type=single_float)
    hidden_state_gradient = hidden_state_gradient + adapter_scale * jnp.dot(backward_down_rows, down_input_factor.T, preferred_element_type=single_float)
    down_input_factor_gradient = adapter_scale * scale_factor * jnp.dot(hidden_state.T, backward_down_rows, preferred_element_type=single_float)
    down_output_factor_gradient = adapter_scale * scale_factor * jnp.dot(lower_down_projection.T, cotangent.astype(single_float), precision=upper_projection)
    sigma = jax.nn.sigmoid(gate)
    gate_back = (hidden_state_gradient * upper * sigma * (1.0 + gate * (1.0 - sigma))).astype(jnp.bfloat16)
    up_back = (hidden_state_gradient * gate * sigma).astype(jnp.bfloat16)
    backward_results = [gate_back, up_back]
    output_factor_gradient = []
    input_factor_gradient = []
    input_total_sum = jnp.zeros(tokens.shape, single_float)
    for rank_dimension in range(2):
        output_factor_gradient.append(adapter_scale * scale_factor * jnp.dot(lower_results[rank_dimension].T, backward_results[rank_dimension].astype(single_float), precision=upper_projection))
        backward_lower_rows = jnp.dot(backward_results[rank_dimension], gate_up_output_factor[rank_dimension].T, preferred_element_type=single_float).astype(jnp.bfloat16)
        input_factor_gradient.append(adapter_scale * scale_factor * jnp.dot(tokens.T, backward_lower_rows, preferred_element_type=single_float))
        input_total_sum = input_total_sum + jnp.dot(backward_results[rank_dimension], gate_up_weight[rank_dimension].T, preferred_element_type=single_float)
        input_total_sum = input_total_sum + adapter_scale * jnp.dot(backward_lower_rows, gate_up_input_factor[rank_dimension].T, preferred_element_type=single_float)
    input_grad = input_total_sum.astype(jnp.bfloat16)
    return (output, input_grad, jnp.stack(input_factor_gradient), jnp.stack(output_factor_gradient), down_input_factor_gradient, down_output_factor_gradient)
```

```python
import jax
import jax.numpy as jnp
from jax import lax
from jax.sharding import PartitionSpec as P


adapter_scale = 2.0
single = jnp.float32
half = jnp.bfloat16
HIGHEST = lax.Precision.HIGHEST


def dot(left, right, dims=((1,), (0,)), precision=None):
    return lax.dot_general(
        left, right, (dims, ((), ())), preferred_element_type=single, precision=precision
    )


def exchange(value, axis, mask):
    size = lax.axis_size(axis)
    return lax.ppermute(value, axis, [(i, i ^ mask) for i in range(size)])


def mp_mask(position, size):
    rest = size // 4
    return (position // rest) | ((position % rest) << 2)


def dp_mask(position, size):
    mask, bits = 0, size.bit_length() - 1
    for bit in range(bits):
        mask = mask | (((position >> (bits - 1 - bit)) & 1) << bit)
    return mask


def owners(axis, total, mask_of):
    size = lax.axis_size(axis)
    rows = total // size
    row = lax.iota(jnp.int32, total)
    block = row // rows
    return (lax.axis_index(axis) ^ mask_of(block, size)) * rows + row % rows


def scatter_mp(partial):
    size = lax.axis_size("mp")
    rest = size // 4
    rows = partial.shape[0] // size
    quarter = rows * rest
    got = [
        exchange(partial[m * quarter : (m + 1) * quarter].astype(half), "mp", m) for m in (1, 2, 3)
    ]
    total = partial[:quarter]
    for piece in got:
        total = total + piece.astype(single)
    while rest > 1:
        rest //= 2
        piece = exchange(total[rest * rows :].astype(half), "mp", rest << 2)
        total = total[: rest * rows] + piece.astype(single)
    return total


def gather_mp(block):
    size = lax.axis_size("mp")
    step = 1
    while step < size // 4:
        block = jnp.concatenate([block, exchange(block, "mp", step << 2)], axis=0)
        step *= 2
    return jnp.concatenate([block] + [exchange(block, "mp", m) for m in (1, 2, 3)], axis=0)


def scatter_dp(partial):
    size = lax.axis_size("dp")
    bit = 1
    while bit < size:
        count = partial.shape[0] // 2
        piece = exchange(partial[count:].astype(half), "dp", bit)
        partial = partial[:count] + piece.astype(single)
        bit *= 2
    return partial


def sum_dp(partial):
    size = lax.axis_size("dp")
    bit = 1
    while bit < size:
        rounded = partial.astype(half)
        partial = rounded.astype(single) + exchange(rounded, "dp", bit).astype(single)
        bit *= 2
    return partial


def per_device(
    tokens,
    gate_up_weight,
    down_weight,
    gate_up_input_factor,
    gate_up_output_factor,
    down_input_factor,
    down_output_factor,
    cotangent,
):
    own, width = tokens.shape
    hidden_width, rank = down_input_factor.shape
    both = lax.all_gather(jnp.concatenate([tokens, cotangent], axis=1), "dp", axis=0, tiled=True)
    total = both.shape[0]
    gradient_scale = adapter_scale * total ** (-0.5)
    mp_token = owners("mp", total, mp_mask)
    dp_token = owners("dp", total, dp_mask)
    to_mp = (mp_token[:, None] == lax.iota(jnp.int32, total)[None, :]).astype(half)
    to_dp = (dp_token[:, None] == mp_token[None, :]).astype(single)
    both = dot(to_mp, both).astype(half)
    x = both[:, :width]
    cot = both[:, width:]

    back_part = dot(cot, down_weight, ((1,), (1,)))
    back_down_part = dot(cot, down_output_factor, ((1,), (1,)))
    low_part = [dot(x, gate_up_input_factor[k]) for k in range(2)]
    back_own = scatter_mp(jnp.concatenate([back_part, back_down_part] + low_part, axis=1))
    pre_part = [dot(x, gate_up_weight[k]) for k in range(2)]
    pre_own = scatter_mp(jnp.concatenate(pre_part, axis=1))

    back_down = back_own[:, hidden_width : hidden_width + rank].astype(half)
    low = [
        back_own[:, hidden_width + (k + 1) * rank : hidden_width + (k + 2) * rank].astype(half)
        for k in range(2)
    ]
    gate, up = [
        pre_own[:, k * hidden_width : (k + 1) * hidden_width]
        + adapter_scale * dot(low[k], gate_up_output_factor[k])
        for k in range(2)
    ]
    hidden = (jax.nn.silu(gate) * up).astype(half)
    hidden_back = back_own[:, :hidden_width] + adapter_scale * dot(
        back_down, down_input_factor, ((1,), (1,))
    )
    sigma = jax.nn.sigmoid(gate)
    gate_back = (hidden_back * up * sigma * (1.0 + gate * (1.0 - sigma))).astype(half)
    up_back = (hidden_back * gate * sigma).astype(half)

    first = gather_mp(jnp.concatenate([hidden, back_down] + low, axis=1))
    second = gather_mp(jnp.concatenate([gate_back, up_back], axis=1))
    hidden_all = first[:, :hidden_width]
    back_down_all = first[:, hidden_width : hidden_width + rank]
    low_all = [
        first[:, hidden_width + (k + 1) * rank : hidden_width + (k + 2) * rank] for k in range(2)
    ]
    back_all = [second[:, k * hidden_width : (k + 1) * hidden_width] for k in range(2)]

    low_down = sum_dp(dot(hidden_all, down_input_factor))
    output_own = scatter_dp(dot(to_dp, dot(hidden_all, down_weight), precision=HIGHEST))
    down_input_factor_gradient = gradient_scale * dot(hidden_all, back_down_all, ((0,), (0,)))
    low_down_own = dot(to_dp[:own], low_down, precision=HIGHEST)
    output = output_own + adapter_scale * dot(
        low_down_own, down_output_factor.astype(single), precision=HIGHEST
    )
    down_output_factor_gradient = gradient_scale * dot(
        low_down, cot.astype(single), ((0,), (0,)), HIGHEST
    )

    gate_up_output_factor_gradient = gradient_scale * jnp.stack(
        [dot(low_all[k], back_all[k], ((0,), (0,))) for k in range(2)]
    )
    back_low = sum_dp(
        jnp.concatenate(
            [dot(back_all[k], gate_up_output_factor[k], ((1,), (1,))) for k in range(2)], axis=1
        )
    ).astype(half)
    grad_gate_up_lower = gradient_scale * jnp.stack(
        [dot(x, back_low[:, k * rank : (k + 1) * rank], ((0,), (0,))) for k in range(2)]
    )
    grad_part = dot(back_all[0], gate_up_weight[0], ((1,), (1,))) + dot(
        back_all[1], gate_up_weight[1], ((1,), (1,))
    )
    grad_own = scatter_dp(dot(to_dp, grad_part, precision=HIGHEST))
    back_low_own = dot(to_dp[:own].astype(half), back_low).astype(half)
    for k in range(2):
        grad_own = grad_own + adapter_scale * dot(
            back_low_own[:, k * rank : (k + 1) * rank], gate_up_input_factor[k], ((1,), (1,))
        )
    return (
        output.astype(half),
        grad_own.astype(half),
        grad_gate_up_lower,
        gate_up_output_factor_gradient,
        down_input_factor_gradient,
        down_output_factor_gradient,
    )


def solution(mesh):
    placed = (
        P("dp", "mp"),
        P(None, "mp", "dp"),
        P("dp", "mp"),
        P(None, "mp", None),
        P(None, None, "dp"),
        P("dp", None),
        P(None, "mp"),
        P("dp", "mp"),
    )
    return jax.shard_map(
        per_device,
        mesh=mesh,
        in_specs=placed,
        out_specs=(
            P("dp", "mp"),
            P("dp", "mp"),
            P(None, "mp", None),
            P(None, None, "dp"),
            P("dp", None),
            P(None, "mp"),
        ),
        check_vma=False,
    )
```

```python
import jax
import jax.numpy as jnp
from jax import lax
from jax.experimental import pallas as pl
from jax.experimental.pallas import tpu as pltpu
from jax.sharding import PartitionSpec as P


adapter_scale = 2.0
single = jnp.float32
half = jnp.bfloat16
HIGHEST = lax.Precision.HIGHEST
vmem_limit = 30 * 2**20
load_limit = 38 * 2**20


def dot(left, right, dims=((1,), (0,)), precision=None):
    return lax.dot_general(
        left, right, (dims, ((), ())), preferred_element_type=single, precision=precision
    )


def exchange(value, axis, mask):
    size = lax.axis_size(axis)
    return lax.ppermute(value, axis, [(i, i ^ mask) for i in range(size)])


def mp_mask(position, size):
    rest = size // 4
    return (position // rest) | ((position % rest) << 2)


def dp_mask(position, size):
    mask, bits = 0, size.bit_length() - 1
    for bit in range(bits):
        mask = mask | (((position >> (bits - 1 - bit)) & 1) << bit)
    return mask


def owners(axis, total, mask_of):
    size = lax.axis_size(axis)
    rows = total // size
    row = lax.iota(jnp.int32, total)
    block = row // rows
    return (lax.axis_index(axis) ^ mask_of(block, size)) * rows + row % rows


def tile(size, limit):
    return max(t for t in range(128, limit + 1, 128) if size % t == 0)


def load(down_weight, gate_up_weight):
    rows, width = down_weight.shape
    depth = gate_up_weight.shape[1]
    parts = 8

    def kernel(down_ref, wide_ref, down_out, gate_out, done):
        copies = []
        for i in range(parts):
            span = pl.ds(i * (rows // parts), rows // parts)
            copies.append(
                pltpu.make_async_copy(down_ref.at[span], down_out.at[span], done.at[0, i])
            )
        for i in range(parts):
            span = pl.ds(i * (depth // parts), depth // parts)
            copies.append(
                pltpu.make_async_copy(wide_ref.at[0, span], gate_out.at[span], done.at[1, i])
            )
        for copy in copies:
            copy.start()
        for copy in copies:
            copy.wait()

    anywhere = pl.BlockSpec(memory_space=pl.ANY)
    return pl.pallas_call(
        kernel,
        in_specs=[anywhere] * 2,
        out_specs=[anywhere] * 2,
        out_shape=[
            jax.ShapeDtypeStruct(down_weight.shape, half),
            jax.ShapeDtypeStruct(gate_up_weight.shape[1:], half),
        ],
        scratch_shapes=[pltpu.SemaphoreType.DMA((2, parts))],
        cost_estimate=pl.CostEstimate(
            flops=10**10, bytes_accessed=4 * rows * (width + depth), transcendentals=0
        ),
        compiler_params=pltpu.CompilerParams(vmem_limit_bytes=load_limit),
    )(down_weight, gate_up_weight)


def project(x, cot, to_true, gate_weight, weight, input_factor, output_factor, hidden):
    total, depth = x.shape
    step = tile(hidden, 768)
    count = hidden // step
    quarter = total // 4
    rows = quarter // 2
    rank = output_factor.shape[0]

    def kernel(*refs):
        x_ref, cot_ref, true_ref, gate_ref, w_ref, in_ref, out_ref = refs[:7]
        near, far, (keep_near, keep_far, low, held, done) = refs[7:10], refs[10:13], refs[13:]

        def fetch(i):
            return pltpu.make_async_copy(
                w_ref.at[1, :, pl.ds(i * step, step)], held.at[i], done.at[i]
            )

        for i in range(count):
            fetch(i).start()
        over = ((1,), (1,))
        parts = [dot(cot_ref[...], out_ref[...], over)]
        parts += [dot(x_ref[...], in_ref[k], over) for k in range(2)]
        for k in range(3):
            low[:, k * rank : (k + 1) * rank] = dot(
                true_ref[...], parts[k].astype(half)
            ).astype(half)
        for i in range(2 * count):
            if i < count:
                block = gate_ref[:, i * step : (i + 1) * step]
            else:
                fetch(i - count).wait()
                block = held[i - count]
            acc = dot(x_ref[...], block)
            span = slice(i * step, (i + 1) * step)
            keep_near[:, span] = acc[:rows]
            keep_far[:, span] = acc[rows:quarter]
            for m in range(1, 4):
                first = acc[m * quarter : m * quarter + rows]
                second = acc[m * quarter + rows : (m + 1) * quarter]
                near[m - 1][:, span] = first.astype(half)
                far[m - 1][:, span] = second.astype(half)

    shape = lambda kind: jax.ShapeDtypeStruct((rows, 2 * hidden), kind)
    vmem = pl.BlockSpec(memory_space=pltpu.VMEM)
    out = pl.pallas_call(
        kernel,
        in_specs=[vmem] * 4 + [pl.BlockSpec(memory_space=pl.ANY)] + [vmem] * 2,
        out_specs=[vmem] * 9,
        out_shape=[shape(half)] * 6
        + [shape(single)] * 2
        + [jax.ShapeDtypeStruct((total, 3 * rank), half)],
        scratch_shapes=[pltpu.VMEM((count, depth, step), half), pltpu.SemaphoreType.DMA((count,))],
        cost_estimate=pl.CostEstimate(
            flops=16 * total * depth * hidden,
            bytes_accessed=4 * depth * hidden,
            transcendentals=0,
        ),
        compiler_params=pltpu.CompilerParams(vmem_limit_bytes=vmem_limit),
    )(x, cot, to_true, gate_weight, weight, input_factor, output_factor)
    return out[:3], out[3:6], out[6], out[7], out[8]


def near_sum(keep, sends):
    got = [exchange(sends[m - 1], "mp", m) for m in (3, 2, 1)]
    return [keep] + [piece.astype(single) for piece in got]


def far_rest(total, rest):
    rows = total.shape[0] // rest
    while rest > 1:
        rest //= 2
        piece = exchange(total[rest * rows :].astype(half), "mp", rest << 2)
        total = total[: rest * rows] + piece.astype(single)
    return total


def gather_rest(block):
    size = lax.axis_size("mp")
    step = 1
    while step < size // 8:
        block = jnp.concatenate([block, exchange(block, "mp", step << 2)], axis=0)
        step *= 2
    return block


def gather_near(block):
    got = {m: exchange(block, "mp", m) for m in (3, 2, 1)}
    return [block] + [got[m] for m in (1, 2, 3)]


def weave(near, far):
    return jnp.concatenate([part for pair in zip(near, far) for part in pair], axis=0)


def scatter_dp(partial):
    size = lax.axis_size("dp")
    bit = 1
    while bit < size:
        count = partial.shape[0] // 2
        piece = partial[count:].astype(half)
        piece = exchange(piece, "dp", bit)
        partial = partial[:count] + piece.astype(single)
        bit *= 2
    return partial


def sum_all(partial, axis):
    size = lax.axis_size(axis)
    bit = 1
    while bit < size:
        rounded = partial.astype(half)
        partial = rounded.astype(single) + exchange(rounded, axis, bit).astype(single)
        bit *= 2
    return partial


def per_device(
    tokens,
    gate_up_weight,
    down_weight,
    gate_up_input_factor,
    gate_up_output_factor,
    down_input_factor,
    down_output_factor,
    cotangent,
):
    own, _ = tokens.shape
    hidden_width, rank = down_input_factor.shape
    block = jnp.concatenate([tokens, cotangent], axis=0)
    dp_size = lax.axis_size("dp")
    pieces = [block] + [exchange(block, "dp", m) for m in range(1, dp_size)]
    down_weight, gate_weight = load(down_weight, gate_up_weight)
    both = jnp.concatenate(pieces, axis=0)
    total = both.shape[0] // 2
    gradient_scale = adapter_scale * total ** (-0.5)
    mp_token = owners("mp", total, mp_mask)
    dp_token = owners("dp", total, dp_mask)
    order = lax.iota(jnp.int32, total)
    row = lax.iota(jnp.int32, 2 * total)
    got_token = (lax.axis_index("dp") ^ (row // (2 * own))) * own + row % own
    got_kind = row // own % 2
    match = mp_token[:, None] == got_token[None, :]
    to_mp = jnp.concatenate(
        [match & (got_kind == kind)[None, :] for kind in range(2)], axis=0
    ).astype(half)
    to_true = (order[:, None] == mp_token[None, :]).astype(half)
    from_true = (mp_token[:, None] == order[None, :]).astype(half)
    to_dp = (dp_token[:, None] == mp_token[None, :]).astype(single)
    own_dp = (dp_token[:own, None] == order[None, :]).astype(single)
    both = dot(to_mp, both).astype(half)
    x = both[:total]
    cot = both[total:]

    back_part = dot(cot, down_weight, ((1,), (1,)))
    quarter = total // 4
    back_sends = [
        back_part[m * quarter : (m + 1) * quarter].astype(half) for m in (1, 2, 3)
    ]
    pre_near, pre_far, pre_near_keep, pre_far_keep, low_part = project(
        x,
        cot,
        to_true,
        gate_weight,
        gate_up_weight,
        jnp.swapaxes(gate_up_input_factor, 1, 2),
        down_output_factor,
        hidden_width,
    )
    low_sum = sum_all(low_part, "mp").astype(half)
    low_sum = dot(from_true, low_sum).astype(half)
    back_down_all = low_sum[:, :rank]
    low_all = [low_sum[:, (k + 1) * rank : (k + 2) * rank] for k in range(2)]

    size = lax.axis_size("mp")
    top = size // 2
    back_parts = near_sum(back_part[:quarter], back_sends)
    pre_parts = near_sum(pre_far_keep, pre_far)
    back_total = sum(back_parts)
    back_crossed = back_total[quarter // 2 :].astype(half)
    pre_crossed = sum(pre_parts).astype(half)
    back_crossed = exchange(back_crossed, "mp", top)
    pre_crossed = exchange(pre_crossed, "mp", top)
    back_own = back_total[: quarter // 2] + back_crossed.astype(single)
    pre_own = sum(near_sum(pre_near_keep, pre_near)) + pre_crossed.astype(single)
    back_own = far_rest(back_own, size // 8)
    pre_own = far_rest(pre_own, size // 8)

    rows = pre_own.shape[0]
    gate, up = [
        pre_own[:, k * hidden_width : (k + 1) * hidden_width]
        + adapter_scale * dot(low_all[k][:rows], gate_up_output_factor[k])
        for k in range(2)
    ]
    hidden = (jax.nn.silu(gate) * up).astype(half)
    hidden_back = back_own + adapter_scale * dot(
        back_down_all[:rows], down_input_factor, ((1,), (1,))
    )
    sigma = jax.nn.sigmoid(gate)
    gate_back = (hidden_back * up * sigma * (1.0 + gate * (1.0 - sigma))).astype(half)
    up_back = (hidden_back * gate * sigma).astype(half)

    block = gather_rest(jnp.concatenate([hidden, gate_back, up_back], axis=1))
    crossed = exchange(block, "mp", top)
    near_block = gather_near(block)
    crossed, near_block[1] = lax.optimization_barrier((crossed, near_block[1]))
    far_hidden = gather_near(crossed[:, :hidden_width])
    far_back = gather_near(crossed[:, hidden_width:])
    hidden_all = weave([piece[:, :hidden_width] for piece in near_block], far_hidden)
    back_all = weave([piece[:, hidden_width:] for piece in near_block], far_back)
    back_all = [back_all[:, k * hidden_width : (k + 1) * hidden_width] for k in range(2)]

    low_down = sum_all(dot(hidden_all, down_input_factor), "dp")
    output_own = scatter_dp(dot(to_dp, dot(hidden_all, down_weight), precision=HIGHEST))
    down_input_factor_gradient = gradient_scale * dot(hidden_all, back_down_all, ((0,), (0,)))
    low_down_own = dot(to_dp[:own], low_down, precision=HIGHEST)
    output = output_own + adapter_scale * dot(
        low_down_own, down_output_factor.astype(single), precision=HIGHEST
    )
    down_output_factor_gradient = gradient_scale * dot(
        low_down, cot.astype(single), ((0,), (0,)), HIGHEST
    )

    gate_up_output_factor_gradient = gradient_scale * jnp.stack(
        [dot(low_all[k], back_all[k], ((0,), (0,))) for k in range(2)]
    )
    back_low = sum_all(
        jnp.concatenate(
            [dot(back_all[k], gate_up_output_factor[k], ((1,), (1,))) for k in range(2)], axis=1
        ),
        "dp",
    ).astype(half)
    grad_gate_up_lower = gradient_scale * jnp.stack(
        [dot(x, back_low[:, k * rank : (k + 1) * rank], ((0,), (0,))) for k in range(2)]
    )
    grad_part = dot(back_all[0], gate_up_weight[0], ((1,), (1,)))
    grad_part = grad_part + dot(back_all[1], gate_up_weight[1], ((1,), (1,)))
    grad_own = scatter_dp(dot(to_dp, grad_part, precision=HIGHEST))
    back_low_own = dot(to_dp[:own].astype(half), back_low).astype(half)
    for k in range(2):
        grad_own = grad_own + adapter_scale * dot(
            back_low_own[:, k * rank : (k + 1) * rank], gate_up_input_factor[k], ((1,), (1,))
        )
    return (
        output.astype(half),
        grad_own.astype(half),
        grad_gate_up_lower,
        gate_up_output_factor_gradient,
        down_input_factor_gradient,
        down_output_factor_gradient,
    )


def solution(mesh):
    placed = (
        P("dp", "mp"),
        P(None, "mp", "dp"),
        P("dp", "mp"),
        P(None, "mp", None),
        P(None, None, "dp"),
        P("dp", None),
        P(None, "mp"),
        P("dp", "mp"),
    )

    return jax.shard_map(
        per_device,
        mesh=mesh,
        in_specs=placed,
        out_specs=(
            P("dp", "mp"),
            P("dp", "mp"),
            P(None, "mp", None),
            P(None, None, "dp"),
            P("dp", None),
            P(None, "mp"),
        ),
        check_vma=False,
    )
```

```python
import jax
import jax.numpy as jnp
from jax import lax
from jax.experimental import pallas as pl
from jax.experimental.pallas import tpu as pltpu
from jax.sharding import PartitionSpec as P


adapter_scale = 2.0
single = jnp.float32
half = jnp.bfloat16
HIGHEST = lax.Precision.HIGHEST
vmem_limit = 30 * 2**20
load_limit = 38 * 2**20


def dot(left, right, dims=((1,), (0,)), precision=None):
    return lax.dot_general(
        left, right, (dims, ((), ())), preferred_element_type=single, precision=precision
    )


def exchange(value, axis, mask):
    size = lax.axis_size(axis)
    return lax.ppermute(value, axis, [(i, i ^ mask) for i in range(size)])


def mp_mask(position, size):
    rest = size // 4
    return (position // rest) | ((position % rest) << 2)


def dp_mask(position, size):
    mask, bits = 0, size.bit_length() - 1
    for bit in range(bits):
        mask = mask | (((position >> (bits - 1 - bit)) & 1) << bit)
    return mask


def owners(axis, total, mask_of):
    size = lax.axis_size(axis)
    rows = total // size
    row = lax.iota(jnp.int32, total)
    block = row // rows
    return (lax.axis_index(axis) ^ mask_of(block, size)) * rows + row % rows


def tile(size, limit):
    return max(t for t in range(128, limit + 1, 128) if size % t == 0)


def load(down_weight, gate_up_weight):
    rows, width = down_weight.shape
    depth = gate_up_weight.shape[1]
    parts = 8

    def kernel(down_ref, wide_ref, down_out, gate_out, done):
        copies = []
        for i in range(parts):
            span = pl.ds(i * (rows // parts), rows // parts)
            copies.append(
                pltpu.make_async_copy(down_ref.at[span], down_out.at[span], done.at[0, i])
            )
        for i in range(parts):
            span = pl.ds(i * (depth // parts), depth // parts)
            copies.append(
                pltpu.make_async_copy(wide_ref.at[0, span], gate_out.at[span], done.at[1, i])
            )
        for copy in copies:
            copy.start()
        for copy in copies:
            copy.wait()

    anywhere = pl.BlockSpec(memory_space=pl.ANY)
    return pl.pallas_call(
        kernel,
        in_specs=[anywhere] * 2,
        out_specs=[anywhere] * 2,
        out_shape=[
            jax.ShapeDtypeStruct(down_weight.shape, half),
            jax.ShapeDtypeStruct(gate_up_weight.shape[1:], half),
        ],
        scratch_shapes=[pltpu.SemaphoreType.DMA((2, parts))],
        cost_estimate=pl.CostEstimate(
            flops=10**10, bytes_accessed=4 * rows * (width + depth), transcendentals=0
        ),
        compiler_params=pltpu.CompilerParams(vmem_limit_bytes=load_limit),
    )(down_weight, gate_up_weight)


def project(x, cot, to_true, gate_weight, weight, input_factor, output_factor, hidden):
    total, depth = x.shape
    step = tile(hidden, 768)
    count = hidden // step
    quarter = total // 4
    rows = quarter // 2
    rank = output_factor.shape[0]

    def kernel(*refs):
        x_ref, cot_ref, true_ref, gate_ref, w_ref, in_ref, out_ref = refs[:7]
        near, far, (keep_near, keep_far, low, held, done) = refs[7:10], refs[10:13], refs[13:]

        def fetch(i):
            return pltpu.make_async_copy(
                w_ref.at[1, :, pl.ds(i * step, step)], held.at[i], done.at[i]
            )

        for i in range(count):
            fetch(i).start()
        over = ((1,), (1,))
        parts = [dot(cot_ref[...], out_ref[...], over)]
        parts += [dot(x_ref[...], in_ref[k], over) for k in range(2)]
        for k in range(3):
            low[:, k * rank : (k + 1) * rank] = dot(
                true_ref[...], parts[k].astype(half)
            ).astype(half)
        for i in range(2 * count):
            if i < count:
                block = gate_ref[:, i * step : (i + 1) * step]
            else:
                fetch(i - count).wait()
                block = held[i - count]
            acc = dot(x_ref[...], block)
            span = slice(i * step, (i + 1) * step)
            keep_near[:, span] = acc[:rows]
            keep_far[:, span] = acc[rows:quarter]
            for m in range(1, 4):
                first = acc[m * quarter : m * quarter + rows]
                second = acc[m * quarter + rows : (m + 1) * quarter]
                near[m - 1][:, span] = first.astype(half)
                far[m - 1][:, span] = second.astype(half)

    shape = lambda kind: jax.ShapeDtypeStruct((rows, 2 * hidden), kind)
    vmem = pl.BlockSpec(memory_space=pltpu.VMEM)
    out = pl.pallas_call(
        kernel,
        in_specs=[vmem] * 4 + [pl.BlockSpec(memory_space=pl.ANY)] + [vmem] * 2,
        out_specs=[vmem] * 9,
        out_shape=[shape(half)] * 6
        + [shape(single)] * 2
        + [jax.ShapeDtypeStruct((total, 3 * rank), half)],
        scratch_shapes=[pltpu.VMEM((count, depth, step), half), pltpu.SemaphoreType.DMA((count,))],
        cost_estimate=pl.CostEstimate(
            flops=16 * total * depth * hidden,
            bytes_accessed=4 * depth * hidden,
            transcendentals=0,
        ),
        compiler_params=pltpu.CompilerParams(vmem_limit_bytes=vmem_limit),
    )(x, cot, to_true, gate_weight, weight, input_factor, output_factor)
    return out[:3], out[3:6], out[6], out[7], out[8]


def near_sum(keep, sends):
    got = [exchange(sends[m - 1], "mp", m) for m in (3, 2, 1)]
    return [keep] + [piece.astype(single) for piece in got]


def far_rest(total, rest):
    rows = total.shape[0] // rest
    while rest > 1:
        rest //= 2
        piece = exchange(total[rest * rows :].astype(half), "mp", rest << 2)
        total = total[: rest * rows] + piece.astype(single)
    return total


def gather_rest(block):
    size = lax.axis_size("mp")
    step = 1
    while step < size // 8:
        block = jnp.concatenate([block, exchange(block, "mp", step << 2)], axis=0)
        step *= 2
    return block


def gather_near(block):
    got = {m: exchange(block, "mp", m) for m in (3, 2, 1)}
    return [block] + [got[m] for m in (1, 2, 3)]


def weave(near, far):
    return jnp.concatenate([part for pair in zip(near, far) for part in pair], axis=0)


def scatter_dp(partial):
    size = lax.axis_size("dp")
    bit = 1
    while bit < size:
        count = partial.shape[0] // 2
        piece = partial[count:].astype(half)
        piece = exchange(piece, "dp", bit)
        partial = partial[:count] + piece.astype(single)
        bit *= 2
    return partial


def sum_all(partial, axis):
    size = lax.axis_size(axis)
    bit = 1
    while bit < size:
        rounded = partial.astype(half)
        partial = rounded.astype(single) + exchange(rounded, axis, bit).astype(single)
        bit *= 2
    return partial


def per_device(
    tokens,
    gate_up_weight,
    down_weight,
    gate_up_input_factor,
    gate_up_output_factor,
    down_input_factor,
    down_output_factor,
    cotangent,
):
    own, _ = tokens.shape
    hidden_width, rank = down_input_factor.shape
    block = jnp.concatenate([tokens, cotangent], axis=0)
    dp_size = lax.axis_size("dp")
    pieces = [block] + [exchange(block, "dp", m) for m in range(1, dp_size)]
    down_weight, gate_weight = load(down_weight, gate_up_weight)
    both = jnp.concatenate(pieces, axis=0)
    total = both.shape[0] // 2
    gradient_scale = adapter_scale * total ** (-0.5)
    mp_token = owners("mp", total, mp_mask)
    dp_token = owners("dp", total, dp_mask)
    order = lax.iota(jnp.int32, total)
    row = lax.iota(jnp.int32, 2 * total)
    got_token = (lax.axis_index("dp") ^ (row // (2 * own))) * own + row % own
    got_kind = row // own % 2
    match = mp_token[:, None] == got_token[None, :]
    to_mp = jnp.concatenate(
        [match & (got_kind == kind)[None, :] for kind in range(2)], axis=0
    ).astype(half)
    to_true = (order[:, None] == mp_token[None, :]).astype(half)
    from_true = (mp_token[:, None] == order[None, :]).astype(half)
    to_dp = (dp_token[:, None] == mp_token[None, :]).astype(single)
    own_dp = (dp_token[:own, None] == order[None, :]).astype(single)
    both = dot(to_mp, both).astype(half)
    x = both[:total]
    cot = both[total:]

    back_part = dot(cot, down_weight, ((1,), (1,)))
    quarter = total // 4
    back_sends = [
        back_part[m * quarter : (m + 1) * quarter].astype(half) for m in (1, 2, 3)
    ]
    pre_near, pre_far, pre_near_keep, pre_far_keep, low_part = project(
        x,
        cot,
        to_true,
        gate_weight,
        gate_up_weight,
        jnp.swapaxes(gate_up_input_factor, 1, 2),
        down_output_factor,
        hidden_width,
    )
    low_sum = sum_all(low_part, "mp").astype(half)
    low_sum = dot(from_true, low_sum).astype(half)
    back_down_all = low_sum[:, :rank]
    low_all = [low_sum[:, (k + 1) * rank : (k + 2) * rank] for k in range(2)]

    size = lax.axis_size("mp")
    top = size // 2
    back_parts = near_sum(back_part[:quarter], back_sends)
    pre_parts = near_sum(pre_far_keep, pre_far)
    back_total = sum(back_parts)
    back_crossed = back_total[quarter // 2 :].astype(half)
    pre_crossed = sum(pre_parts).astype(half)
    back_crossed = exchange(back_crossed, "mp", top)
    pre_crossed = exchange(pre_crossed, "mp", top)
    back_own = back_total[: quarter // 2] + back_crossed.astype(single)
    pre_own = sum(near_sum(pre_near_keep, pre_near)) + pre_crossed.astype(single)
    back_own = far_rest(back_own, size // 8)
    pre_own = far_rest(pre_own, size // 8)

    rows = pre_own.shape[0]
    gate, up = [
        pre_own[:, k * hidden_width : (k + 1) * hidden_width]
        + adapter_scale * dot(low_all[k][:rows], gate_up_output_factor[k])
        for k in range(2)
    ]
    hidden = (jax.nn.silu(gate) * up).astype(half)
    hidden_back = back_own + adapter_scale * dot(
        back_down_all[:rows], down_input_factor, ((1,), (1,))
    )
    sigma = jax.nn.sigmoid(gate)
    gate_back = (hidden_back * up * sigma * (1.0 + gate * (1.0 - sigma))).astype(half)
    up_back = (hidden_back * gate * sigma).astype(half)

    block = gather_rest(jnp.concatenate([hidden, gate_back, up_back], axis=1))
    crossed = exchange(block, "mp", top)
    near_block = gather_near(block)
    crossed, near_block[1] = lax.optimization_barrier((crossed, near_block[1]))
    far_hidden = gather_near(crossed[:, :hidden_width])
    far_back = gather_near(crossed[:, hidden_width:])
    hidden_all = weave([piece[:, :hidden_width] for piece in near_block], far_hidden)
    back_all = weave([piece[:, hidden_width:] for piece in near_block], far_back)
    back_all = [back_all[:, k * hidden_width : (k + 1) * hidden_width] for k in range(2)]

    low_down = sum_all(dot(hidden_all, down_input_factor), "dp")
    output_own = scatter_dp(dot(to_dp, dot(hidden_all, down_weight), precision=HIGHEST))
    down_input_factor_gradient = gradient_scale * dot(hidden_all, back_down_all, ((0,), (0,)))
    low_down_own = dot(to_dp[:own], low_down, precision=HIGHEST)
    output = output_own + adapter_scale * dot(
        low_down_own, down_output_factor.astype(single), precision=HIGHEST
    )
    down_output_factor_gradient = gradient_scale * dot(
        low_down, cot.astype(single), ((0,), (0,)), HIGHEST
    )

    factor_parts = jnp.stack([dot(low_all[k], back_all[k], ((0,), (0,))) for k in range(2)])
    gate_up_output_factor_gradient = gradient_scale * factor_parts
    back_low = sum_all(
        jnp.concatenate(
            [dot(back_all[k], gate_up_output_factor[k], ((1,), (1,))) for k in range(2)], axis=1
        ),
        "dp",
    ).astype(half)
    grad_gate_up_lower = gradient_scale * jnp.stack(
        [dot(x, back_low[:, k * rank : (k + 1) * rank], ((0,), (0,))) for k in range(2)]
    )
    grad_part = dot(back_all[0], gate_up_weight[0], ((1,), (1,)))
    grad_part = grad_part + dot(back_all[1], gate_up_weight[1], ((1,), (1,)))
    grad_own = scatter_dp(dot(to_dp, grad_part, precision=HIGHEST))
    back_low_own = dot(to_dp[:own].astype(half), back_low).astype(half)
    for k in range(2):
        grad_own = grad_own + adapter_scale * dot(
            back_low_own[:, k * rank : (k + 1) * rank], gate_up_input_factor[k], ((1,), (1,))
        )
    return (
        output.astype(half),
        grad_own.astype(half),
        grad_gate_up_lower,
        gate_up_output_factor_gradient,
        down_input_factor_gradient,
        down_output_factor_gradient,
    )


def solution(mesh):
    placed = (
        P("dp", "mp"),
        P(None, "mp", "dp"),
        P("dp", "mp"),
        P(None, "mp", None),
        P(None, None, "dp"),
        P("dp", None),
        P(None, "mp"),
        P("dp", "mp"),
    )

    return jax.shard_map(
        per_device,
        mesh=mesh,
        in_specs=placed,
        out_specs=(
            P("dp", "mp"),
            P("dp", "mp"),
            P(None, "mp", None),
            P(None, None, "dp"),
            P("dp", None),
            P(None, "mp"),
        ),
        check_vma=False,
    )
```
